32 devices in a mesh: groups: 2 (over x), docs: 16 (over z, y, core).
Axes of the slice: x: 2, y: 2, z: 4, core: 2. Of those that a mesh axis runs over, the one named last changes fastest.
Arguments:
- sentences: bfloat16 [65536, 1280], P(('groups', 'docs')), parts along dimension 0, may hold values from -10 to 10
- sent_doc: int32 [65536], P('groups'), parts along dimension 0, may hold values from 0 to 2047, never falling along the last dimension, each value on 1 to 32 neighbouring positions
- images: bfloat16 [8192, 1280], P(('groups', 'docs')), parts along dimension 0, may hold values from -30 to 30
- image_owner: int32 [8192, 1], P(('groups', 'docs')), parts along dimension 0, may hold values from 0 to 15, as said below
- anchor: int32 [8192], P(('groups', 'docs')), parts along dimension 0, may hold values from 0 to 2047, as said below
- loader_shard: int32 [8192, 1], P(('groups', 'docs')), parts along dimension 0, may hold values from 0 to 15, as said below
Outputs:
- loaded_images: bfloat16 [16384, 1280], P(('groups', 'docs')), parts along dimension 0
- loaded_text: bfloat16 [16384, 1280], P(('groups', 'docs')), parts along dimension 0
The draws below stay inside these ranges and needn't reach their ends.
There are 2 independent parts, one for each index of `groups`. The reference program is written for one: setup_inputs(seed, part) draws one part's arguments, and reference() takes and returns one part's arrays. A program takes and returns all parts, laid end to end along the dimension named above; each array names one. Nothing has to cross between parts.
Inputs may be any that keep to these rules, and one draw needn't show every extreme that they name: `sent_doc`: documents are runs of 1 to 32 consecutive sentences, ids never falling. `image_owner`: the 256 images of one device name one owner at most 32 times, and some owner exactly 32 times. loader_shard = (a[source device] + b[image_owner]) mod 16 for two permutations a and b of the devices, drawn with the data. So the images of one device name one shard at most 32 times (some exactly 32), and the images that one owner receives from all devices name one shard at most 32 times, all from one source device. `anchor`: the image's document is the document of this sentence of its owner.
All inputs are finite; a program needn't handle non-finite values.
Results may differ from the reference program's by a relative error of at most 0.0048.
Values may be sent and summed in bfloat16 or wider, within the bound.
A program may use at most 64 MiB of HBM per device.

```python
import math
import jax
import jax.numpy as jnp
import numpy as np
from jax import lax

E = 1280
S_DEV = 2048
I_DEV = 256
MOST_SENT = 32
CAP = 32
SENTS = 32768
IMAGES = 4096
DOCS = 2048
SLOTS = 8192
N_DOCS = 16


def draw_sentences(key, part):
    base = jnp.clip(jax.random.normal(jax.random.fold_in(key, 11), (SENTS, E), jnp.float32), -6.0, 6.0)
    return base.astype(jnp.bfloat16)


def draw_images(key, part):
    base = jnp.clip(jax.random.normal(jax.random.fold_in(key, 13), (IMAGES, E), jnp.float32), -6.0, 6.0)
    return base.astype(jnp.bfloat16)


def draw_anchor(key, part):
    chooser = jax.random.randint(jax.random.fold_in(key, 21), (IMAGES,), 0, 4)
    nearby = jax.random.randint(jax.random.fold_in(key, 23), (IMAGES,), 0, 2 * MOST_SENT)
    edges = jnp.where(nearby < MOST_SENT, nearby, S_DEV - 2 * MOST_SENT + nearby)
    spread = jax.random.randint(jax.random.fold_in(key, 29), (IMAGES,), 0, S_DEV)
    return jnp.where(chooser == 0, edges, spread).astype(jnp.int32)


def route_pair(key):
    base = jax.random.fold_in(key, 31)
    listing = jnp.repeat(jnp.arange(N_DOCS, dtype=jnp.int32), CAP)
    total = N_DOCS * CAP
    leaning = jax.random.randint(jax.random.fold_in(base, 1), (N_DOCS,), 0, 3)
    chosen = jax.random.randint(jax.random.fold_in(base, 2), (N_DOCS,), 0, N_DOCS)
    noise = jax.random.randint(jax.random.fold_in(base, 3), (N_DOCS, total), 0, 4096)
    score = noise + leaning[listing][None, :] * 4096 + 1
    score = jnp.where(listing[None, :] == chosen[:, None], 0, score)
    score = score * total + jnp.arange(total, dtype=jnp.int32)[None, :]
    order = jnp.argsort(score, axis=1)
    owners = listing[order[:, :I_DEV]]
    spot_score = jax.random.randint(jax.random.fold_in(base, 4), (N_DOCS, I_DEV), 0, 4096) * I_DEV + jnp.arange(I_DEV, dtype=jnp.int32)[None, :]
    owners = jnp.take_along_axis(owners, jnp.argsort(spot_score, axis=1), axis=1)
    first_perm = jax.random.permutation(jax.random.fold_in(base, 5), N_DOCS).astype(jnp.int32)
    second_perm = jax.random.permutation(jax.random.fold_in(base, 6), N_DOCS).astype(jnp.int32)
    shards = (first_perm[:, None] + second_perm[owners]) % N_DOCS
    return (owners.reshape(IMAGES, 1).astype(jnp.int32), shards.reshape(IMAGES, 1).astype(jnp.int32))


def draw_image_owner(key, part):
    return route_pair(key)[0]


def draw_loader_shard(key, part):
    return route_pair(key)[1]


def profile(count, total, limit, skew):
    portions = [(1 << 20) // math.isqrt(rank ** skew) + 1 for rank in range(2, count + 1)]
    spare, holding = total - limit - (count - 1), [1] * (count - 1)
    while spare > 0:
        candidates = [i for i in range(count - 1) if holding[i] < limit]
        mass, budget = sum([portions[i] for i in candidates]), spare
        for i in candidates:
            more = min(limit - holding[i], max(1, budget * portions[i] // mass), spare)
            holding[i] = holding[i] + more
            spare = spare - more
    return np.array([limit] + holding)


def ragged(key, number_of, total, most, lean):
    if number_of == 2:
        one = jax.random.randint(key, (), max(1, total - most), min(most, total - 1) + 1)
        return jnp.stack([one, total - one])
    sizes = jnp.asarray(profile(number_of, total, most, lean), jnp.int32)
    pairs = (number_of - 1) // 2
    donor, receiver = sizes[1:1 + 2 * pairs:2], sizes[2:2 + 2 * pairs:2]
    room = jnp.minimum(donor - 1, most - receiver)
    shifted = jax.random.randint(jax.random.fold_in(key, 1), (pairs,), 0, 1 << 20) % (room + 1)
    sizes = sizes.at[1:1 + 2 * pairs:2].set(donor - shifted).at[2:2 + 2 * pairs:2].set(receiver + shifted)
    return sizes[jax.random.permutation(jax.random.fold_in(key, 2), number_of)]


def setup_inputs(seed: int = 0, part: int = 0) -> dict:
    streams_of = jax.random.split(jax.random.key(seed), 7)
    part_splits = jax.random.split(jax.random.fold_in(streams_of[6], part), 7)
    return {
        "sentences": draw_sentences(jax.random.fold_in(jax.random.fold_in(streams_of[6], part), 71), part),
        "sent_doc": jnp.searchsorted(jnp.cumsum(ragged(part_splits[1], DOCS, SENTS, MOST_SENT, 1)), jnp.arange(SENTS), side="right").astype(jnp.int32),
        "images": draw_images(jax.random.fold_in(jax.random.fold_in(streams_of[6], part), 71), part),
        "image_owner": draw_image_owner(jax.random.fold_in(jax.random.fold_in(streams_of[6], part), 71), part),
        "anchor": draw_anchor(jax.random.fold_in(jax.random.fold_in(streams_of[6], part), 71), part),
        "loader_shard": draw_loader_shard(jax.random.fold_in(jax.random.fold_in(streams_of[6], part), 71), part),
    }


def reference(sentences, sent_doc, images, image_owner, anchor, loader_shard):
    temper = E ** -0.5
    reach = MOST_SENT
    padded = jnp.pad(sentences, ((reach, reach), (0, 0)))
    padded_ids = jnp.pad(sent_doc, (reach, reach), constant_values=-1)
    centre = (image_owner[:, 0] * S_DEV + anchor).astype(jnp.int32)
    doc_ids = sent_doc[centre]
    offsets = jnp.arange(2 * reach + 1, dtype=jnp.int32)

    def align_block(pieces):
        queries, middle, owned = pieces
        indices = middle[:, None] + offsets[None, :]
        window = padded[indices].astype(jnp.float32)
        window_ids = padded_ids[indices]
        scores = jnp.einsum("be,bwe->bw", queries.astype(jnp.float32), window) * temper
        member = window_ids == owned[:, None]
        peak = jnp.max(jnp.where(member, scores, -1e30), axis=1, keepdims=True)
        raised = jnp.where(member, jnp.exp(scores - peak), 0.0)
        denominator = jnp.sum(raised, axis=1, keepdims=True)
        weights = (raised / denominator).astype(jnp.bfloat16)
        return jnp.einsum("bw,bwe->be", weights.astype(jnp.float32), window).astype(jnp.bfloat16)

    aligned = lax.map(align_block, (images.reshape(N_DOCS, I_DEV, E), centre.reshape(N_DOCS, I_DEV), doc_ids.reshape(N_DOCS, I_DEV)))
    aligned = aligned.reshape(IMAGES, E)
    targets = loader_shard[:, 0]
    sources = jnp.arange(IMAGES, dtype=jnp.int32) // I_DEV
    labels = jnp.arange(N_DOCS, dtype=jnp.int32)
    onehot = (targets[:, None] == labels[None, :]).astype(jnp.int32).reshape(N_DOCS, I_DEV, N_DOCS)
    ranking = jnp.sum((jnp.cumsum(onehot, axis=1) - 1) * onehot, axis=2).reshape(IMAGES)
    places = (targets * (N_DOCS * CAP) + sources * CAP + ranking).astype(jnp.int32)
    loaded_images = jnp.zeros((SLOTS, E), jnp.bfloat16).at[places].set(images)
    loaded_text = jnp.zeros((SLOTS, E), jnp.bfloat16).at[places].set(aligned)
    return loaded_images, loaded_text
```

```python
import functools

import jax
import jax.numpy as jnp
from jax import lax
from jax.experimental import pallas as pl
from jax.experimental.pallas import tpu as pltpu
from jax.sharding import PartitionSpec as P

MOST_SENT = 32
LANES = 128
SUB = 8
MESH = pl.DeviceIdType.MESH
HIGH = lax.Precision.HIGHEST
TRANS_LHS = (((0,), (0,)), ((), ()))
TRANS_RHS = (((1,), (1,)), ((), ()))


def iota(shape, dim):
    return lax.broadcasted_iota(jnp.int32, shape, dim)


def exchange_kernel(
    n, cap, block, tile, cols_ref, images_ref, ids_ref, sent_ref,
    img_out, txt_out, meta_out,
    ext, disp, shrd, arrived, aligned, tsend, meta_s, target_ref,
    local_sem, halo_send, halo_recv, send_sem, recv_sem,
):
    me = lax.axis_index("docs")
    own_rows, feature = sent_ref.shape
    width = ext.shape[0]
    count = images_ref.shape[0]
    rows = n * block
    temper = feature ** (-0.5)

    barrier = pltpu.get_barrier_semaphore()

    @pl.loop(1, n)
    def _(k):
        pl.semaphore_signal(barrier, inc=1, device_id={"docs": lax.rem(me + k, n)}, device_id_type=MESH)

    load = pltpu.make_async_copy(sent_ref, ext.at[pl.ds(MOST_SENT, own_rows)], local_sem.at[0])
    load.start()

    owner, anchor, shard = cols_ref[:, 0:1], cols_ref[:, 1:2], cols_ref[:, 2:3]
    wide = max(LANES, n)
    onehot = (owner == iota((count, wide), 1)).astype(jnp.float32)
    below = (iota((count, count), 0) > iota((count, count), 1)).astype(jnp.bfloat16)
    counts = jnp.dot(below, onehot.astype(jnp.bfloat16), preferred_element_type=jnp.float32)
    rank = jnp.sum(counts * onehot, axis=1, keepdims=True).astype(jnp.int32)
    lane = iota((count, LANES), 1)
    first = rank == 0
    for_owner = jnp.where(lane == rank, anchor + 1, 0) + jnp.where((lane == cap) & first, shard + 1, 0)
    for_shard = jnp.where((lane == cap + 1) & first, owner + 1, 0)
    keyed = iota((count, n * SUB), 1)
    meta = lax.dot_general(
        (keyed == owner * SUB).astype(jnp.float32), for_owner.astype(jnp.float32), TRANS_LHS,
        precision=HIGH, preferred_element_type=jnp.float32,
    ) + lax.dot_general(
        (keyed == shard * SUB).astype(jnp.float32), for_shard.astype(jnp.float32), TRANS_LHS,
        precision=HIGH, preferred_element_type=jnp.float32,
    )
    meta_s[...] = meta.astype(jnp.int32)

    def fill(ref, key):
        place = key * block + rank

        @pl.loop(0, rows // tile)
        def _(t):
            base = pl.multiple_of(t * tile, tile)
            table = (place == iota((count, tile), 1) + base).astype(jnp.bfloat16)
            ref[pl.ds(base, tile), :] = lax.dot_general(
                table, images_ref[...], TRANS_LHS, preferred_element_type=jnp.float32
            ).astype(jnp.bfloat16)

    fill(disp, owner)
    fill(shrd, shard)
    pl.semaphore_wait(barrier, n - 1)

    def at(ref, who, size):
        return ref.at[pl.ds(pl.multiple_of(who * size, size), size)]

    def remote(kind, src, dst, size, peer, slot):
        return pltpu.make_async_remote_copy(
            src_ref=at(src, peer, size), dst_ref=at(dst, slot, size),
            send_sem=send_sem.at[kind, peer], recv_sem=recv_sem.at[kind, slot],
            device_id={"docs": peer}, device_id_type=MESH,
        )

    flows = ((meta_s, meta_out, SUB), (disp, arrived, block), (shrd, img_out, block), (tsend, txt_out, block))

    def start(kind):
        src, dst, size = flows[kind]

        @pl.loop(1, n)
        def _(k):
            remote(kind, src, dst, size, lax.rem(me + k, n), me).start()

        pltpu.make_async_copy(at(src, me, size), at(dst, me, size), local_sem.at[1 + kind]).start()

    def finish(kind, sent):
        src, dst, size = flows[kind]

        @pl.loop(1, n)
        def _(k):
            peer = lax.rem(me + k, n)
            if sent:
                remote(kind, src, dst, size, peer, me).wait_send()
            else:
                remote(kind, src, dst, size, peer, peer).wait_recv()

        if not sent:
            pltpu.make_async_copy(at(src, me, size), at(dst, me, size), local_sem.at[1 + kind]).wait()

    def halo(way):
        to = lax.rem(me + 1, n) if way == 0 else lax.rem(me + n - 1, n)
        src = own_rows - MOST_SENT if way == 0 else 0
        dst = 0 if way == 0 else own_rows + MOST_SENT
        return pltpu.make_async_remote_copy(
            src_ref=sent_ref.at[pl.ds(src, MOST_SENT)], dst_ref=ext.at[pl.ds(dst, MOST_SENT)],
            send_sem=halo_send.at[way], recv_sem=halo_recv.at[way],
            device_id={"docs": to}, device_id_type=MESH,
        )

    start(0)
    halo(0).start()
    halo(1).start()
    start(1)
    start(2)
    load.wait()
    for way in (0, 1):
        halo(way).wait_recv()
    finish(0, False)
    finish(1, False)

    ids = ids_ref[...]
    records = meta_out[...].astype(jnp.float32)

    @pl.loop(0, rows // tile)
    def _(t):
        base = pl.multiple_of(t * tile, tile)
        spot = iota((tile, n * SUB), 0) + base
        picker = (lax.div(spot, block) * SUB == iota((tile, n * SUB), 1)).astype(jnp.float32)
        picked = jnp.dot(picker, records, precision=HIGH, preferred_element_type=jnp.float32)
        picked = picked.astype(jnp.int32)
        step = lax.rem(iota((tile, 1), 0) + base, block)
        lanes = iota((tile, LANES), 1)
        anchored = jnp.sum(jnp.where((lanes == step) & (lanes < cap), picked, 0), axis=1, keepdims=True)
        goal = jnp.sum(jnp.where(lanes == cap, picked, 0), axis=1, keepdims=True)
        target_ref[pl.ds(base, tile), :] = (goal - 1) * block + step
        filled = anchored > 0
        here = iota((tile, width), 1) == anchored - 1 + MOST_SENT
        doc = jnp.sum(jnp.where(here, ids, 0), axis=1, keepdims=True)
        doc = jnp.where(filled, doc, -2)
        scores = lax.dot_general(
            arrived[pl.ds(base, tile), :], ext[...], TRANS_RHS, preferred_element_type=jnp.float32
        ) * temper
        member = doc == ids
        peak = jnp.max(jnp.where(member, scores, -1e30), axis=1, keepdims=True)
        raised = jnp.where(member, jnp.exp(scores - peak), 0.0)
        total = jnp.sum(raised, axis=1, keepdims=True)
        weights = (raised / jnp.where(filled, total, 1.0)).astype(jnp.bfloat16)
        aligned[pl.ds(base, tile), :] = jnp.dot(
            weights, ext[...], preferred_element_type=jnp.float32
        ).astype(jnp.bfloat16)

    @pl.loop(0, rows // tile)
    def _(t):
        base = pl.multiple_of(t * tile, tile)
        table = (target_ref[...] == iota((rows, tile), 1) + base).astype(jnp.bfloat16)
        tsend[pl.ds(base, tile), :] = lax.dot_general(
            table, aligned[...], TRANS_LHS, preferred_element_type=jnp.float32
        ).astype(jnp.bfloat16)

    start(3)
    for way in (0, 1):
        halo(way).wait_send()
    finish(0, True)
    finish(1, True)
    finish(2, True)
    finish(2, False)
    finish(3, True)
    finish(3, False)


def place_kernel(n, block, lane, meta_ref, img_ref, txt_ref, img_out, txt_out, buf, sems):
    copy = pltpu.make_async_copy(img_ref, img_out, sems.at[0])
    copy.start()
    for s in range(n):
        source = meta_ref[s * SUB, lane]
        rows = txt_ref[pl.ds(pl.multiple_of(jnp.maximum(source - 1, 0) * block, block), block), :]
        buf[pl.ds(s * block, block), :] = jnp.where(source > 0, rows, jnp.zeros_like(rows))
        pltpu.make_async_copy(
            buf.at[pl.ds(s * block, block)], txt_out.at[pl.ds(s * block, block)], sems.at[1 + s]
        ).start()
    for s in range(n):
        pltpu.make_async_copy(
            buf.at[pl.ds(s * block, block)], txt_out.at[pl.ds(s * block, block)], sems.at[1 + s]
        ).wait()
    copy.wait()


def shards(sentences, sent_doc, images, image_owner, anchor, loader_shard):
    n = lax.axis_size("docs")
    me = lax.axis_index("docs")
    own_rows, feature = sentences.shape
    count = images.shape[0]
    cap = max(4, 2 * count // n)
    block = -(-cap // 16) * 16
    rows = n * block
    tile = min(256, rows)
    width = own_rows + 2 * MOST_SENT
    padded_ids = jnp.pad(sent_doc, (MOST_SENT, MOST_SENT), constant_values=-1)
    ids = lax.dynamic_slice_in_dim(padded_ids, me * own_rows, width)[None, :]
    cols = jnp.concatenate([image_owner, anchor[:, None], loader_shard], axis=1)
    half = jax.ShapeDtypeStruct((rows, feature), jnp.bfloat16)
    slots = pltpu.VMEM((rows, feature), jnp.bfloat16)
    dma = pltpu.SemaphoreType.DMA
    vmem = pl.BlockSpec(memory_space=pltpu.VMEM)
    got_img, got_txt, meta = pl.pallas_call(
        functools.partial(exchange_kernel, n, cap, block, tile),
        out_shape=(half, half, jax.ShapeDtypeStruct((n * SUB, LANES), jnp.int32)),
        in_specs=[vmem, vmem, vmem, pl.BlockSpec(memory_space=pl.ANY)],
        out_specs=(vmem, vmem, vmem),
        scratch_shapes=[
            pltpu.VMEM((width, feature), jnp.bfloat16),
            slots, slots, slots, slots, slots,
            pltpu.VMEM((n * SUB, LANES), jnp.int32),
            pltpu.VMEM((rows, 1), jnp.int32),
            dma((5,)), dma((2,)), dma((2,)), dma((4, n)), dma((4, n)),
        ],
        compiler_params=pltpu.CompilerParams(
            collective_id=0, has_side_effects=True, vmem_limit_bytes=60 * 1024 * 1024
        ),
    )(cols, images, ids, sentences)
    if block != cap:
        meta = meta.reshape(n, SUB, LANES)[:, 0, cap + 1]
        picked = got_txt.reshape(n, block, feature)[jnp.maximum(meta - 1, 0), :cap]
        text = jnp.where((meta > 0)[:, None, None], picked, jnp.zeros_like(picked))
        image = got_img.reshape(n, block, feature)[:, :cap]
        return (image.reshape(n * cap, feature), text.reshape(n * cap, feature))
    return pl.pallas_call(
        functools.partial(place_kernel, n, block, cap + 1),
        out_shape=(half, half),
        in_specs=[pl.BlockSpec(memory_space=pltpu.SMEM), vmem, vmem],
        out_specs=(pl.BlockSpec(memory_space=pl.ANY), pl.BlockSpec(memory_space=pl.ANY)),
        scratch_shapes=[slots, dma((1 + n,))],
    )(meta, got_img, got_txt)


def solution(mesh):
    return jax.shard_map(
        shards,
        mesh=mesh,
        in_specs=(
            P(("groups", "docs"), None),
            P("groups"),
            P(("groups", "docs"), None),
            P(("groups", "docs"), None),
            P(("groups", "docs")),
            P(("groups", "docs"), None),
        ),
        out_specs=(P(("groups", "docs"), None), P(("groups", "docs"), None)),
        check_vma=False,
    )
```

```python
import functools

import jax
import jax.numpy as jnp
from jax import lax
from jax.experimental import pallas as pl
from jax.experimental.pallas import tpu as pltpu
from jax.sharding import PartitionSpec as P

MOST_SENT = 32
LANES = 128
SUB = 8
MESH = pl.DeviceIdType.MESH
HIGH = lax.Precision.HIGHEST
TRANS_LHS = (((0,), (0,)), ((), ()))
TRANS_RHS = (((1,), (1,)), ((), ()))


def iota(shape, dim):
    return lax.broadcasted_iota(jnp.int32, shape, dim)


def ranks(keys, n):
    count = keys.shape[1]
    onehot = (keys == iota((n, count), 0)).astype(jnp.float32)
    above = (iota((count, count), 0) < iota((count, count), 1)).astype(jnp.bfloat16)
    counts = jnp.dot(onehot.astype(jnp.bfloat16), above, preferred_element_type=jnp.float32)
    return jnp.sum(counts * onehot, axis=0, keepdims=True).astype(jnp.int32)


def exchange_kernel(
    n, cap, block, tile, rows_ref, images_ref, ids_ref, sent_ref,
    img_out, txt_out, meta_out,
    ext, far_images, far_rows, disp, shrd, far_disp, far_shrd, arrived, aligned, tsend, meta_s, target_ref,
    local_sem, halo_send, halo_recv, raw_send, raw_recv, send_sem, recv_sem,
):
    me = lax.axis_index("docs")
    half = n // 2
    first = lax.div(me, half) * half
    across = lax.rem(first + half, n)
    partner = lax.rem(me + half, n)
    own_rows, feature = sent_ref.shape
    width = ext.shape[0]
    count = images_ref.shape[0]
    rows = n * block
    part = half * block
    temper = feature ** (-0.5)

    barrier = pltpu.get_barrier_semaphore()

    @pl.loop(1, n)
    def _(k):
        pl.semaphore_signal(barrier, inc=1, device_id={"docs": lax.rem(me + k, n)}, device_id_type=MESH)

    load = pltpu.make_async_copy(sent_ref, ext.at[pl.ds(MOST_SENT, own_rows)], local_sem.at[0])
    load.start()
    pl.semaphore_wait(barrier, n - 1)

    def raw(which):
        src, dst = ((rows_ref, far_rows), (images_ref, far_images))[which]
        return pltpu.make_async_remote_copy(
            src_ref=src, dst_ref=dst, send_sem=raw_send.at[which], recv_sem=raw_recv.at[which],
            device_id={"docs": partner}, device_id_type=MESH,
        )

    def halo(way):
        to = lax.rem(me + 1, n) if way == 0 else lax.rem(me + n - 1, n)
        src = own_rows - MOST_SENT if way == 0 else 0
        dst = 0 if way == 0 else own_rows + MOST_SENT
        return pltpu.make_async_remote_copy(
            src_ref=sent_ref.at[pl.ds(src, MOST_SENT)], dst_ref=ext.at[pl.ds(dst, MOST_SENT)],
            send_sem=halo_send.at[way], recv_sem=halo_recv.at[way],
            device_id={"docs": to}, device_id_type=MESH,
        )

    halo(0).start()
    halo(1).start()
    raw(0).start()
    raw(1).start()

    owner, anchor, shard = rows_ref[0:1, :], rows_ref[1:2, :], rows_ref[2:3, :]
    rank = ranks(owner, n)
    lane = iota((LANES, count), 0)
    lead = rank == 0
    for_owner = jnp.where(lane == rank, anchor + 1, 0) + jnp.where((lane == cap) & lead, shard + 1, 0)
    for_shard = jnp.where((lane == cap + 1) & lead, owner + 1, 0)
    keyed = iota((n * SUB, count), 0)
    meta = lax.dot_general(
        (keyed == owner * SUB).astype(jnp.float32), for_owner.astype(jnp.float32), TRANS_RHS,
        precision=HIGH, preferred_element_type=jnp.float32,
    ) + lax.dot_general(
        (keyed == shard * SUB).astype(jnp.float32), for_shard.astype(jnp.float32), TRANS_RHS,
        precision=HIGH, preferred_element_type=jnp.float32,
    )
    meta_s[...] = meta.astype(jnp.int32)

    def fill(ref, key, order, values):
        place = key * block + order

        @pl.loop(0, part // tile)
        def _(t):
            base = pl.multiple_of(t * tile, tile)
            table = (place == iota((tile, count), 0) + (base + first * block)).astype(jnp.bfloat16)
            ref[pl.ds(base, tile), :] = jnp.dot(
                table, values[...], preferred_element_type=jnp.float32
            ).astype(jnp.bfloat16)

    fill(disp, owner, rank, images_ref)
    fill(shrd, shard, rank, images_ref)

    def at(ref, who, size):
        return ref.at[pl.ds(pl.multiple_of(who * size, size), size)]

    flows = (
        (meta_s, meta_out, SUB, True, False),
        (disp, arrived, block, False, False),
        (shrd, img_out, block, False, False),
        (tsend, txt_out, block, True, False),
        (far_disp, arrived, block, False, True),
        (far_shrd, img_out, block, False, True),
    )

    def remote(kind, peer, sender):
        src, dst, size, everyone, far = flows[kind]
        piece = peer if everyone else lax.rem(peer, half)
        slot = lax.rem(sender + half, n) if far else sender
        return pltpu.make_async_remote_copy(
            src_ref=at(src, piece, size), dst_ref=at(dst, slot, size),
            send_sem=send_sem.at[kind, peer], recv_sem=recv_sem.at[kind, sender],
            device_id={"docs": peer}, device_id_type=MESH,
        )

    def local(kind):
        src, dst, size, everyone, far = flows[kind]
        piece = me if everyone else me - first
        slot = partner if far else me
        return pltpu.make_async_copy(at(src, piece, size), at(dst, slot, size), local_sem.at[1 + kind])

    def each(kind, act):
        if flows[kind][3]:

            @pl.loop(0, half)
            def _(k):
                act(across + lax.rem(me - first + k, half))

        @pl.loop(1, half)
        def _(k):
            act(first + lax.rem(me - first + k, half))

    def start(kind):
        each(kind, lambda peer: remote(kind, peer, me).start())
        local(kind).start()

    def sent(kind):
        each(kind, lambda peer: remote(kind, peer, me).wait_send())

    def landed(kind):
        each(kind, lambda peer: remote(kind, peer, peer).wait_recv())
        local(kind).wait()

    start(0)
    start(1)
    start(2)
    load.wait()
    for way in (0, 1):
        halo(way).wait_recv()
    landed(0)
    ids = ids_ref[...]
    records = meta_out[...].astype(jnp.float32)

    def align(head):
        @pl.loop(0, part // tile)
        def _(t):
            base = pl.multiple_of(head * block + t * tile, tile)
            spot = iota((tile, n * SUB), 0) + base
            picker = (lax.div(spot, block) * SUB == iota((tile, n * SUB), 1)).astype(jnp.float32)
            picked = jnp.dot(picker, records, precision=HIGH, preferred_element_type=jnp.float32)
            picked = picked.astype(jnp.int32)
            step = lax.rem(iota((tile, 1), 0) + base, block)
            lanes = iota((tile, LANES), 1)
            anchored = jnp.sum(jnp.where((lanes == step) & (lanes < cap), picked, 0), axis=1, keepdims=True)
            goal = jnp.sum(jnp.where(lanes == cap, picked, 0), axis=1, keepdims=True)
            target_ref[pl.ds(base, tile), :] = (goal - 1) * block + step
            filled = anchored > 0
            here = iota((tile, width), 1) == anchored - 1 + MOST_SENT
            doc = jnp.sum(jnp.where(here, ids, 0), axis=1, keepdims=True)
            doc = jnp.where(filled, doc, -2)
            scores = lax.dot_general(
                arrived[pl.ds(base, tile), :], ext[...], TRANS_RHS, preferred_element_type=jnp.float32
            ) * temper
            member = doc == ids
            peak = jnp.max(jnp.where(member, scores, -1e30), axis=1, keepdims=True)
            raised = jnp.where(member, jnp.exp(scores - peak), 0.0)
            total = jnp.sum(raised, axis=1, keepdims=True)
            weights = (raised / jnp.where(filled, total, 1.0)).astype(jnp.bfloat16)
            aligned[pl.ds(base, tile), :] = jnp.dot(
                weights, ext[...], preferred_element_type=jnp.float32
            ).astype(jnp.bfloat16)

    def route(head, more):
        begin = pl.multiple_of(head * block, part)

        @pl.loop(0, rows // tile)
        def _(t):
            base = pl.multiple_of(t * tile, tile)
            table = target_ref[pl.ds(begin, part), :] == iota((part, tile), 1) + base
            moved = lax.dot_general(
                table.astype(jnp.bfloat16), aligned[pl.ds(begin, part), :], TRANS_LHS,
                preferred_element_type=jnp.float32,
            ).astype(jnp.bfloat16)
            if more:
                moved = tsend[pl.ds(base, tile), :] + moved
            tsend[pl.ds(base, tile), :] = moved

    landed(1)
    align(first)
    route(first, False)
    raw(0).wait_recv()
    far_owner, far_shard = far_rows[0:1, :], far_rows[2:3, :]
    far_rank = ranks(far_owner, n)
    raw(1).wait_recv()
    fill(far_disp, far_owner, far_rank, far_images)
    fill(far_shrd, far_shard, far_rank, far_images)
    start(4)
    start(5)
    landed(4)
    align(across)
    route(across, True)
    start(3)
    for way in (0, 1):
        halo(way).wait_send()
        raw(way).wait_send()
    for kind in (0, 1, 2, 4, 5):
        sent(kind)
    landed(2)
    landed(5)
    sent(3)
    landed(3)


def place_kernel(n, block, lane, meta_ref, img_ref, txt_ref, img_out, txt_out, buf, sems):
    copy = pltpu.make_async_copy(img_ref, img_out, sems.at[0])
    copy.start()
    for s in range(n):
        source = meta_ref[s * SUB, lane]
        rows = txt_ref[pl.ds(pl.multiple_of(jnp.maximum(source - 1, 0) * block, block), block), :]
        buf[pl.ds(s * block, block), :] = jnp.where(source > 0, rows, jnp.zeros_like(rows))
        pltpu.make_async_copy(
            buf.at[pl.ds(s * block, block)], txt_out.at[pl.ds(s * block, block)], sems.at[1 + s]
        ).start()
    for s in range(n):
        pltpu.make_async_copy(
            buf.at[pl.ds(s * block, block)], txt_out.at[pl.ds(s * block, block)], sems.at[1 + s]
        ).wait()
    copy.wait()


def shards(sentences, sent_doc, images, image_owner, anchor, loader_shard):
    n = lax.axis_size("docs")
    me = lax.axis_index("docs")
    own_rows, feature = sentences.shape
    count = images.shape[0]
    cap = max(4, 2 * count // n)
    block = -(-cap // 16) * 16
    rows = n * block
    tile = min(256, rows // 2)
    width = own_rows + 2 * MOST_SENT
    padded_ids = jnp.pad(sent_doc, (MOST_SENT, MOST_SENT), constant_values=-1)
    ids = lax.dynamic_slice_in_dim(padded_ids, me * own_rows, width)[None, :]
    blank = jnp.zeros((SUB - 3, count), jnp.int32)
    table = jnp.concatenate([image_owner.T, anchor[None, :], loader_shard.T, blank], axis=0)
    half = jax.ShapeDtypeStruct((rows, feature), jnp.bfloat16)
    slots = pltpu.VMEM((rows, feature), jnp.bfloat16)
    some = pltpu.VMEM((rows // 2, feature), jnp.bfloat16)
    anywhere = pl.BlockSpec(memory_space=pl.ANY)
    dma = pltpu.SemaphoreType.DMA
    vmem = pl.BlockSpec(memory_space=pltpu.VMEM)
    got_img, got_txt, meta = pl.pallas_call(
        functools.partial(exchange_kernel, n, cap, block, tile),
        out_shape=(half, half, jax.ShapeDtypeStruct((n * SUB, LANES), jnp.int32)),
        in_specs=[vmem, vmem, vmem, anywhere],
        out_specs=(anywhere, anywhere, vmem),
        scratch_shapes=[
            pltpu.VMEM((width, feature), jnp.bfloat16),
            pltpu.VMEM((count, feature), jnp.bfloat16),
            pltpu.VMEM((SUB, count), jnp.int32),
            some, some, some, some, slots, slots, slots,
            pltpu.VMEM((n * SUB, LANES), jnp.int32),
            pltpu.VMEM((rows, 1), jnp.int32),
            dma((7,)), dma((2,)), dma((2,)), dma((2,)), dma((2,)), dma((6, n)), dma((6, n)),
        ],
        compiler_params=pltpu.CompilerParams(
            collective_id=0, has_side_effects=True, vmem_limit_bytes=60 * 1024 * 1024
        ),
    )(table, images, ids, sentences)
    if block != cap:
        meta = meta.reshape(n, SUB, LANES)[:, 0, cap + 1]
        picked = got_txt.reshape(n, block, feature)[jnp.maximum(meta - 1, 0), :cap]
        text = jnp.where((meta > 0)[:, None, None], picked, jnp.zeros_like(picked))
        image = got_img.reshape(n, block, feature)[:, :cap]
        return (image.reshape(n * cap, feature), text.reshape(n * cap, feature))
    return pl.pallas_call(
        functools.partial(place_kernel, n, block, cap + 1),
        out_shape=(half, half),
        in_specs=[pl.BlockSpec(memory_space=pltpu.SMEM), vmem, vmem],
        out_specs=(anywhere, anywhere),
        scratch_shapes=[slots, dma((1 + n,))],
    )(meta, got_img, got_txt)


def solution(mesh):
    return jax.shard_map(
        shards,
        mesh=mesh,
        in_specs=(
            P(("groups", "docs"), None),
            P("groups"),
            P(("groups", "docs"), None),
            P(("groups", "docs"), None),
            P(("groups", "docs")),
            P(("groups", "docs"), None),
        ),
        out_specs=(P(("groups", "docs"), None), P(("groups", "docs"), None)),
        check_vma=False,
    )
```

```python
import functools

import jax
import jax.numpy as jnp
from jax import lax
from jax.experimental import pallas as pl
from jax.experimental.pallas import tpu as pltpu
from jax.sharding import PartitionSpec as P

MOST_SENT = 32
LANES = 128
SUB = 8
MESH = pl.DeviceIdType.MESH
HIGH = lax.Precision.HIGHEST
TRANS_LHS = (((0,), (0,)), ((), ()))
TRANS_RHS = (((1,), (1,)), ((), ()))


def iota(shape, dim):
    return lax.broadcasted_iota(jnp.int32, shape, dim)


def ranks(keys, n):
    count = keys.shape[1]
    onehot = (keys == iota((n, count), 0)).astype(jnp.float32)
    above = (iota((count, count), 0) < iota((count, count), 1)).astype(jnp.bfloat16)
    counts = jnp.dot(onehot.astype(jnp.bfloat16), above, preferred_element_type=jnp.float32)
    return jnp.sum(counts * onehot, axis=0, keepdims=True).astype(jnp.int32)


def exchange_kernel(
    n, cap, block, tile, owner_ref, anchor_ref, shard_ref, images_ref, ids_ref, sent_ref,
    img_out, txt_out, meta_out,
    ext, far_images, far_owner_ref, far_shard_ref, disp, shrd, far_disp, far_shrd, arrived, aligned, tsend, meta_s, target_ref,
    local_sem, halo_send, halo_recv, raw_send, raw_recv, send_sem, recv_sem,
):
    me = lax.axis_index("docs")
    half = n // 2
    first = lax.div(me, half) * half
    across = lax.rem(first + half, n)
    partner = lax.rem(me + half, n)
    own_rows, feature = sent_ref.shape
    width = ext.shape[0]
    count = images_ref.shape[0]
    rows = n * block
    part = half * block
    temper = feature ** (-0.5)

    barrier = pltpu.get_barrier_semaphore()

    @pl.loop(1, n)
    def _(k):
        pl.semaphore_signal(barrier, inc=1, device_id={"docs": lax.rem(me + k, n)}, device_id_type=MESH)

    load = pltpu.make_async_copy(sent_ref, ext.at[pl.ds(MOST_SENT, own_rows)], local_sem.at[0])
    load.start()
    pl.semaphore_wait(barrier, n - 1)

    def raw(which):
        src, dst = ((owner_ref, far_owner_ref), (shard_ref, far_shard_ref), (images_ref, far_images))[which]
        return pltpu.make_async_remote_copy(
            src_ref=src, dst_ref=dst, send_sem=raw_send.at[which], recv_sem=raw_recv.at[which],
            device_id={"docs": partner}, device_id_type=MESH,
        )

    def halo(way):
        to = lax.rem(me + 1, n) if way == 0 else lax.rem(me + n - 1, n)
        src = own_rows - MOST_SENT if way == 0 else 0
        dst = 0 if way == 0 else own_rows + MOST_SENT
        return pltpu.make_async_remote_copy(
            src_ref=sent_ref.at[pl.ds(src, MOST_SENT)], dst_ref=ext.at[pl.ds(dst, MOST_SENT)],
            send_sem=halo_send.at[way], recv_sem=halo_recv.at[way],
            device_id={"docs": to}, device_id_type=MESH,
        )

    halo(0).start()
    halo(1).start()
    for which in range(3):
        raw(which).start()

    owner, anchor, shard = owner_ref[...], anchor_ref[...], shard_ref[...]
    rank = ranks(owner, n)
    lane = iota((LANES, count), 0)
    lead = rank == 0
    for_owner = jnp.where(lane == rank, anchor + 1, 0) + jnp.where((lane == cap) & lead, shard + 1, 0)
    for_shard = jnp.where((lane == cap + 1) & lead, owner + 1, 0)
    keyed = iota((n * SUB, count), 0)
    meta = lax.dot_general(
        (keyed == owner * SUB).astype(jnp.float32), for_owner.astype(jnp.float32), TRANS_RHS,
        precision=HIGH, preferred_element_type=jnp.float32,
    ) + lax.dot_general(
        (keyed == shard * SUB).astype(jnp.float32), for_shard.astype(jnp.float32), TRANS_RHS,
        precision=HIGH, preferred_element_type=jnp.float32,
    )
    meta_s[...] = meta.astype(jnp.int32)

    def fill(ref, key, order, values):
        place = key * block + order

        @pl.loop(0, part // tile)
        def _(t):
            base = pl.multiple_of(t * tile, tile)
            table = (place == iota((tile, count), 0) + (base + first * block)).astype(jnp.bfloat16)
            ref[pl.ds(base, tile), :] = jnp.dot(
                table, values[...], preferred_element_type=jnp.float32
            ).astype(jnp.bfloat16)

    fill(disp, owner, rank, images_ref)
    fill(shrd, shard, rank, images_ref)

    def at(ref, who, size):
        return ref.at[pl.ds(pl.multiple_of(who * size, size), size)]

    flows = (
        (meta_s, meta_out, SUB, True, False),
        (disp, arrived, block, False, False),
        (shrd, img_out, block, False, False),
        (tsend, txt_out, block, True, False),
        (far_disp, arrived, block, False, True),
        (far_shrd, img_out, block, False, True),
    )

    def remote(kind, peer, sender):
        src, dst, size, everyone, far = flows[kind]
        piece = peer if everyone else lax.rem(peer, half)
        slot = lax.rem(sender + half, n) if far else sender
        return pltpu.make_async_remote_copy(
            src_ref=at(src, piece, size), dst_ref=at(dst, slot, size),
            send_sem=send_sem.at[kind, peer], recv_sem=recv_sem.at[kind, sender],
            device_id={"docs": peer}, device_id_type=MESH,
        )

    def local(kind):
        src, dst, size, everyone, far = flows[kind]
        piece = me if everyone else me - first
        slot = partner if far else me
        return pltpu.make_async_copy(at(src, piece, size), at(dst, slot, size), local_sem.at[1 + kind])

    def each(kind, act):
        if flows[kind][3]:

            @pl.loop(0, half)
            def _(k):
                act(across + lax.rem(me - first + k, half))

        @pl.loop(1, half)
        def _(k):
            act(first + lax.rem(me - first + k, half))

    def start(kind):
        each(kind, lambda peer: remote(kind, peer, me).start())
        local(kind).start()

    def sent(kind):
        each(kind, lambda peer: remote(kind, peer, me).wait_send())

    def landed(kind):
        each(kind, lambda peer: remote(kind, peer, peer).wait_recv())
        local(kind).wait()

    start(0)
    start(1)
    start(2)
    load.wait()
    for way in (0, 1):
        halo(way).wait_recv()
    landed(0)
    ids = ids_ref[...]
    records = meta_out[...].astype(jnp.float32)

    def align(head):
        @pl.loop(0, part // tile)
        def _(t):
            base = pl.multiple_of(head * block + t * tile, tile)
            spot = iota((tile, n * SUB), 0) + base
            picker = (lax.div(spot, block) * SUB == iota((tile, n * SUB), 1)).astype(jnp.float32)
            picked = jnp.dot(picker, records, precision=HIGH, preferred_element_type=jnp.float32)
            picked = picked.astype(jnp.int32)
            step = lax.rem(iota((tile, 1), 0) + base, block)
            lanes = iota((tile, LANES), 1)
            anchored = jnp.sum(jnp.where((lanes == step) & (lanes < cap), picked, 0), axis=1, keepdims=True)
            goal = jnp.sum(jnp.where(lanes == cap, picked, 0), axis=1, keepdims=True)
            target_ref[pl.ds(base, tile), :] = (goal - 1) * block + step
            filled = anchored > 0
            here = iota((tile, width), 1) == anchored - 1 + MOST_SENT
            doc = jnp.sum(jnp.where(here, ids, 0), axis=1, keepdims=True)
            doc = jnp.where(filled, doc, -2)
            scores = lax.dot_general(
                arrived[pl.ds(base, tile), :], ext[...], TRANS_RHS, preferred_element_type=jnp.float32
            ) * temper
            member = doc == ids
            peak = jnp.max(jnp.where(member, scores, -1e30), axis=1, keepdims=True)
            raised = jnp.where(member, jnp.exp(scores - peak), 0.0)
            total = jnp.sum(raised, axis=1, keepdims=True)
            weights = (raised / jnp.where(filled, total, 1.0)).astype(jnp.bfloat16)
            aligned[pl.ds(base, tile), :] = jnp.dot(
                weights, ext[...], preferred_element_type=jnp.float32
            ).astype(jnp.bfloat16)

    def route(head, more):
        begin = pl.multiple_of(head * block, part)

        @pl.loop(0, rows // tile)
        def _(t):
            base = pl.multiple_of(t * tile, tile)
            table = target_ref[pl.ds(begin, part), :] == iota((part, tile), 1) + base
            moved = lax.dot_general(
                table.astype(jnp.bfloat16), aligned[pl.ds(begin, part), :], TRANS_LHS,
                preferred_element_type=jnp.float32,
            ).astype(jnp.bfloat16)
            if more:
                moved = tsend[pl.ds(base, tile), :] + moved
            tsend[pl.ds(base, tile), :] = moved

    landed(1)
    align(first)
    route(first, False)
    raw(0).wait_recv()
    raw(1).wait_recv()
    far_owner, far_shard = far_owner_ref[...], far_shard_ref[...]
    far_rank = ranks(far_owner, n)
    raw(2).wait_recv()
    fill(far_disp, far_owner, far_rank, far_images)
    start(4)
    fill(far_shrd, far_shard, far_rank, far_images)
    sent(4)
    landed(4)
    start(5)
    align(across)
    route(across, True)
    start(3)
    for way in (0, 1):
        halo(way).wait_send()
    for which in range(3):
        raw(which).wait_send()
    for kind in (0, 1, 2, 5):
        sent(kind)
    landed(2)
    landed(5)
    sent(3)
    landed(3)


def place_kernel(n, block, lane, meta_ref, img_ref, txt_ref, img_out, txt_out, buf, sems):
    copy = pltpu.make_async_copy(img_ref, img_out, sems.at[0])
    copy.start()
    for s in range(n):
        source = meta_ref[s * SUB, lane]
        rows = txt_ref[pl.ds(pl.multiple_of(jnp.maximum(source - 1, 0) * block, block), block), :]
        buf[pl.ds(s * block, block), :] = jnp.where(source > 0, rows, jnp.zeros_like(rows))
        pltpu.make_async_copy(
            buf.at[pl.ds(s * block, block)], txt_out.at[pl.ds(s * block, block)], sems.at[1 + s]
        ).start()
    for s in range(n):
        pltpu.make_async_copy(
            buf.at[pl.ds(s * block, block)], txt_out.at[pl.ds(s * block, block)], sems.at[1 + s]
        ).wait()
    copy.wait()


def shards(sentences, sent_doc, images, image_owner, anchor, loader_shard):
    n = lax.axis_size("docs")
    me = lax.axis_index("docs")
    own_rows, feature = sentences.shape
    count = images.shape[0]
    cap = max(4, 2 * count // n)
    block = -(-cap // 16) * 16
    rows = n * block
    tile = min(256, rows // 2)
    width = own_rows + 2 * MOST_SENT
    padded_ids = jnp.pad(sent_doc, (MOST_SENT, MOST_SENT), constant_values=-1)
    ids = lax.dynamic_slice_in_dim(padded_ids, me * own_rows, width)[None, :]
    half = jax.ShapeDtypeStruct((rows, feature), jnp.bfloat16)
    slots = pltpu.VMEM((rows, feature), jnp.bfloat16)
    some = pltpu.VMEM((rows // 2, feature), jnp.bfloat16)
    anywhere = pl.BlockSpec(memory_space=pl.ANY)
    dma = pltpu.SemaphoreType.DMA
    vmem = pl.BlockSpec(memory_space=pltpu.VMEM)
    got_img, got_txt, meta = pl.pallas_call(
        functools.partial(exchange_kernel, n, cap, block, tile),
        out_shape=(half, half, jax.ShapeDtypeStruct((n * SUB, LANES), jnp.int32)),
        in_specs=[vmem] * 5 + [anywhere],
        out_specs=(anywhere, anywhere, vmem),
        scratch_shapes=[
            pltpu.VMEM((width, feature), jnp.bfloat16),
            pltpu.VMEM((count, feature), jnp.bfloat16),
            pltpu.VMEM((1, count), jnp.int32),
            pltpu.VMEM((1, count), jnp.int32),
            some, some, some, some, slots, slots, slots,
            pltpu.VMEM((n * SUB, LANES), jnp.int32),
            pltpu.VMEM((rows, 1), jnp.int32),
            dma((7,)), dma((2,)), dma((2,)), dma((3,)), dma((3,)), dma((6, n)), dma((6, n)),
        ],
        compiler_params=pltpu.CompilerParams(
            collective_id=0, has_side_effects=True, vmem_limit_bytes=60 * 1024 * 1024
        ),
    )(image_owner.T, anchor[None, :], loader_shard.T, images, ids, sentences)
    if block != cap:
        meta = meta.reshape(n, SUB, LANES)[:, 0, cap + 1]
        picked = got_txt.reshape(n, block, feature)[jnp.maximum(meta - 1, 0), :cap]
        text = jnp.where((meta > 0)[:, None, None], picked, jnp.zeros_like(picked))
        image = got_img.reshape(n, block, feature)[:, :cap]
        return (image.reshape(n * cap, feature), text.reshape(n * cap, feature))
    return pl.pallas_call(
        functools.partial(place_kernel, n, block, cap + 1),
        out_shape=(half, half),
        in_specs=[pl.BlockSpec(memory_space=pltpu.SMEM), vmem, vmem],
        out_specs=(anywhere, anywhere),
        scratch_shapes=[slots, dma((1 + n,))],
    )(meta, got_img, got_txt)


def solution(mesh):
    return jax.shard_map(
        shards,
        mesh=mesh,
        in_specs=(
            P(("groups", "docs"), None),
            P("groups"),
            P(("groups", "docs"), None),
            P(("groups", "docs"), None),
            P(("groups", "docs")),
            P(("groups", "docs"), None),
        ),
        out_specs=(P(("groups", "docs"), None), P(("groups", "docs"), None)),
        check_vma=False,
    )
```

```python
import functools

import jax
import jax.numpy as jnp
from jax import lax
from jax.experimental import pallas as pl
from jax.experimental.pallas import tpu as pltpu
from jax.sharding import PartitionSpec as P

MOST_SENT = 32
LANES = 128
SUB = 8
MESH = pl.DeviceIdType.MESH
HIGH = lax.Precision.HIGHEST
TRANS_LHS = (((0,), (0,)), ((), ()))
TRANS_RHS = (((1,), (1,)), ((), ()))


def iota(shape, dim):
    return lax.broadcasted_iota(jnp.int32, shape, dim)


def ranks(keys, n):
    count = keys.shape[1]
    onehot = (keys == iota((n, count), 0)).astype(jnp.float32)
    above = (iota((count, count), 0) < iota((count, count), 1)).astype(jnp.bfloat16)
    counts = jnp.dot(onehot.astype(jnp.bfloat16), above, preferred_element_type=jnp.float32)
    return jnp.sum(counts * onehot, axis=0, keepdims=True).astype(jnp.int32)


def exchange_kernel(
    n, cap, block, tile, owner_ref, anchor_ref, shard_ref, images_ref, ids_ref, sent_ref,
    img_out, txt_out, meta_out,
    ext, far_images, far_owner_ref, far_shard_ref, disp, shrd, far_disp, far_shrd, arrived, aligned, tsend, meta_s, target_ref,
    local_sem, halo_send, halo_recv, raw_send, raw_recv, send_sem, recv_sem,
):
    me = lax.axis_index("docs")
    half = n // 2
    first = lax.div(me, half) * half
    across = lax.rem(first + half, n)
    partner = lax.rem(me + half, n)
    own_rows, feature = sent_ref.shape
    width = ext.shape[0]
    count = images_ref.shape[0]
    rows = n * block
    part = half * block
    temper = feature ** (-0.5)

    barrier = pltpu.get_barrier_semaphore()

    @pl.loop(1, n)
    def _(k):
        pl.semaphore_signal(barrier, inc=1, device_id={"docs": lax.rem(me + k, n)}, device_id_type=MESH)

    load = pltpu.make_async_copy(sent_ref, ext.at[pl.ds(MOST_SENT, own_rows)], local_sem.at[0])
    load.start()
    pl.semaphore_wait(barrier, n - 1)

    def raw(which):
        src, dst = ((owner_ref, far_owner_ref), (shard_ref, far_shard_ref), (images_ref, far_images))[which]
        return pltpu.make_async_remote_copy(
            src_ref=src, dst_ref=dst, send_sem=raw_send.at[which], recv_sem=raw_recv.at[which],
            device_id={"docs": partner}, device_id_type=MESH,
        )

    def halo(way):
        to = lax.rem(me + 1, n) if way == 0 else lax.rem(me + n - 1, n)
        src = own_rows - MOST_SENT if way == 0 else 0
        dst = 0 if way == 0 else own_rows + MOST_SENT
        return pltpu.make_async_remote_copy(
            src_ref=sent_ref.at[pl.ds(src, MOST_SENT)], dst_ref=ext.at[pl.ds(dst, MOST_SENT)],
            send_sem=halo_send.at[way], recv_sem=halo_recv.at[way],
            device_id={"docs": to}, device_id_type=MESH,
        )

    halo(0).start()
    halo(1).start()
    for which in range(3):
        raw(which).start()

    owner, anchor, shard = owner_ref[...], anchor_ref[...], shard_ref[...]
    rank = ranks(owner, n)
    lane = iota((LANES, count), 0)
    lead = rank == 0
    for_owner = jnp.where(lane == rank, anchor + 1, 0) + jnp.where((lane == cap) & lead, shard + 1, 0)
    for_shard = jnp.where((lane == cap + 1) & lead, owner + 1, 0)
    keyed = iota((n * SUB, count), 0)
    meta = lax.dot_general(
        (keyed == owner * SUB).astype(jnp.float32), for_owner.astype(jnp.float32), TRANS_RHS,
        precision=HIGH, preferred_element_type=jnp.float32,
    ) + lax.dot_general(
        (keyed == shard * SUB).astype(jnp.float32), for_shard.astype(jnp.float32), TRANS_RHS,
        precision=HIGH, preferred_element_type=jnp.float32,
    )
    meta_s[...] = meta.astype(jnp.int32)

    def fill(ref, key, order, values):
        place = key * block + order

        @pl.loop(0, part // tile)
        def _(t):
            base = pl.multiple_of(t * tile, tile)
            table = (place == iota((tile, count), 0) + (base + first * block)).astype(jnp.bfloat16)
            ref[pl.ds(base, tile), :] = jnp.dot(
                table, values[...], preferred_element_type=jnp.float32
            ).astype(jnp.bfloat16)

    fill(disp, owner, rank, images_ref)
    fill(shrd, shard, rank, images_ref)

    def at(ref, who, size):
        return ref.at[pl.ds(pl.multiple_of(who * size, size), size)]

    flows = (
        (meta_s, meta_out, SUB, True, False),
        (disp, arrived, block, False, False),
        (shrd, img_out, block, False, False),
        (tsend, txt_out, block, True, False),
        (far_disp, arrived, block, False, True),
        (far_shrd, img_out, block, False, True),
    )

    def remote(kind, peer, sender):
        src, dst, size, everyone, far = flows[kind]
        piece = peer if everyone else lax.rem(peer, half)
        slot = lax.rem(sender + half, n) if far else sender
        return pltpu.make_async_remote_copy(
            src_ref=at(src, piece, size), dst_ref=at(dst, slot, size),
            send_sem=send_sem.at[kind, peer], recv_sem=recv_sem.at[kind, sender],
            device_id={"docs": peer}, device_id_type=MESH,
        )

    def local(kind):
        src, dst, size, everyone, far = flows[kind]
        piece = me if everyone else me - first
        slot = partner if far else me
        return pltpu.make_async_copy(at(src, piece, size), at(dst, slot, size), local_sem.at[1 + kind])

    def each(kind, act):
        if flows[kind][3]:

            @pl.loop(0, half)
            def _(k):
                act(across + lax.rem(me - first + k, half))

        @pl.loop(1, half)
        def _(k):
            act(first + lax.rem(me - first + k, half))

    def start(kind):
        each(kind, lambda peer: remote(kind, peer, me).start())
        local(kind).start()

    def sent(kind):
        each(kind, lambda peer: remote(kind, peer, me).wait_send())

    def landed(kind):
        each(kind, lambda peer: remote(kind, peer, peer).wait_recv())
        local(kind).wait()

    start(0)
    start(1)
    start(2)
    load.wait()
    for way in (0, 1):
        halo(way).wait_recv()
    landed(0)
    ids = ids_ref[...]
    records = meta_out[...].astype(jnp.float32)

    def align(head):
        @pl.loop(0, part // tile)
        def _(t):
            base = pl.multiple_of(head * block + t * tile, tile)
            spot = iota((tile, n * SUB), 0) + base
            picker = (lax.div(spot, block) * SUB == iota((tile, n * SUB), 1)).astype(jnp.float32)
            picked = jnp.dot(picker, records, precision=HIGH, preferred_element_type=jnp.float32)
            picked = picked.astype(jnp.int32)
            step = lax.rem(iota((tile, 1), 0) + base, block)
            lanes = iota((tile, LANES), 1)
            anchored = jnp.sum(jnp.where((lanes == step) & (lanes < cap), picked, 0), axis=1, keepdims=True)
            goal = jnp.sum(jnp.where(lanes == cap, picked, 0), axis=1, keepdims=True)
            target_ref[pl.ds(base, tile), :] = (goal - 1) * block + step
            filled = anchored > 0
            here = iota((tile, width), 1) == anchored - 1 + MOST_SENT
            doc = jnp.sum(jnp.where(here, ids, 0), axis=1, keepdims=True)
            doc = jnp.where(filled, doc, -2)
            scores = lax.dot_general(
                arrived[pl.ds(base, tile), :], ext[...], TRANS_RHS, preferred_element_type=jnp.float32
            ) * temper
            member = doc == ids
            peak = jnp.max(jnp.where(member, scores, -1e30), axis=1, keepdims=True)
            raised = jnp.where(member, jnp.exp(scores - peak), 0.0)
            total = jnp.sum(raised, axis=1, keepdims=True)
            weights = (raised / jnp.where(filled, total, 1.0)).astype(jnp.bfloat16)
            aligned[pl.ds(base, tile), :] = jnp.dot(
                weights, ext[...], preferred_element_type=jnp.float32
            ).astype(jnp.bfloat16)

    def route(head, more):
        begin = pl.multiple_of(head * block, part)

        @pl.loop(0, rows // tile)
        def _(t):
            base = pl.multiple_of(t * tile, tile)
            table = target_ref[pl.ds(begin, part), :] == iota((part, tile), 1) + base
            moved = lax.dot_general(
                table.astype(jnp.bfloat16), aligned[pl.ds(begin, part), :], TRANS_LHS,
                preferred_element_type=jnp.float32,
            ).astype(jnp.bfloat16)
            if more:
                moved = tsend[pl.ds(base, tile), :] + moved
            tsend[pl.ds(base, tile), :] = moved

    landed(1)
    align(first)
    route(first, False)
    raw(0).wait_recv()
    raw(1).wait_recv()
    far_owner, far_shard = far_owner_ref[...], far_shard_ref[...]
    far_rank = ranks(far_owner, n)
    raw(2).wait_recv()
    fill(far_disp, far_owner, far_rank, far_images)
    start(4)
    fill(far_shrd, far_shard, far_rank, far_images)
    sent(4)
    landed(4)
    start(5)
    align(across)
    route(across, True)
    start(3)
    for way in (0, 1):
        halo(way).wait_send()
    for which in range(3):
        raw(which).wait_send()
    for kind in (0, 1, 2, 5):
        sent(kind)
    landed(2)
    landed(5)
    sent(3)
    landed(3)


def place_kernel(n, block, lane, meta_ref, img_ref, txt_ref, img_out, txt_out, img_buf, txt_buf, sems):
    def at(ref, who):
        return ref.at[pl.ds(pl.multiple_of(who * block, block), block)]

    def picked(s):
        source = jnp.maximum(meta_ref[s * SUB, lane] - 1, 0)
        return pltpu.make_async_copy(at(txt_ref, source), at(txt_buf, s), sems.at[1, s])

    for s in range(n):
        picked(s).start()
        pltpu.make_async_copy(at(img_ref, s), at(img_buf, s), sems.at[0, s]).start()
    for s in range(n):
        picked(s).wait()

        @pl.when(meta_ref[s * SUB, lane] <= 0)
        def _():
            txt_buf[pl.ds(s * block, block), :] = jnp.zeros((block, txt_buf.shape[1]), txt_buf.dtype)

        pltpu.make_async_copy(at(img_ref, s), at(img_buf, s), sems.at[0, s]).wait()
        pltpu.make_async_copy(at(img_buf, s), at(img_out, s), sems.at[2, s]).start()
    for s in range(n):
        pltpu.make_async_copy(at(txt_buf, s), at(txt_out, s), sems.at[3, s]).start()
    for s in range(n):
        pltpu.make_async_copy(at(txt_buf, s), at(txt_out, s), sems.at[3, s]).wait()
        pltpu.make_async_copy(at(img_buf, s), at(img_out, s), sems.at[2, s]).wait()


def shards(sentences, sent_doc, images, image_owner, anchor, loader_shard):
    n = lax.axis_size("docs")
    me = lax.axis_index("docs")
    own_rows, feature = sentences.shape
    count = images.shape[0]
    cap = max(4, 2 * count // n)
    block = -(-cap // 16) * 16
    rows = n * block
    tile = min(256, rows // 2)
    width = own_rows + 2 * MOST_SENT
    padded_ids = jnp.pad(sent_doc, (MOST_SENT, MOST_SENT), constant_values=-1)
    ids = lax.dynamic_slice_in_dim(padded_ids, me * own_rows, width)[None, :]
    half = jax.ShapeDtypeStruct((rows, feature), jnp.bfloat16)
    slots = pltpu.VMEM((rows, feature), jnp.bfloat16)
    some = pltpu.VMEM((rows // 2, feature), jnp.bfloat16)
    anywhere = pl.BlockSpec(memory_space=pl.ANY)
    dma = pltpu.SemaphoreType.DMA
    vmem = pl.BlockSpec(memory_space=pltpu.VMEM)
    got_img, got_txt, meta = pl.pallas_call(
        functools.partial(exchange_kernel, n, cap, block, tile),
        out_shape=(half, half, jax.ShapeDtypeStruct((n * SUB, LANES), jnp.int32)),
        in_specs=[vmem] * 5 + [anywhere],
        out_specs=(anywhere, anywhere, vmem),
        scratch_shapes=[
            pltpu.VMEM((width, feature), jnp.bfloat16),
            pltpu.VMEM((count, feature), jnp.bfloat16),
            pltpu.VMEM((1, count), jnp.int32),
            pltpu.VMEM((1, count), jnp.int32),
            some, some, some, some, slots, slots, slots,
            pltpu.VMEM((n * SUB, LANES), jnp.int32),
            pltpu.VMEM((rows, 1), jnp.int32),
            dma((7,)), dma((2,)), dma((2,)), dma((3,)), dma((3,)), dma((6, n)), dma((6, n)),
        ],
        compiler_params=pltpu.CompilerParams(
            collective_id=0, has_side_effects=True, vmem_limit_bytes=60 * 1024 * 1024
        ),
    )(image_owner.T, anchor[None, :], loader_shard.T, images, ids, sentences)
    if block != cap:
        meta = meta.reshape(n, SUB, LANES)[:, 0, cap + 1]
        picked = got_txt.reshape(n, block, feature)[jnp.maximum(meta - 1, 0), :cap]
        text = jnp.where((meta > 0)[:, None, None], picked, jnp.zeros_like(picked))
        image = got_img.reshape(n, block, feature)[:, :cap]
        return (image.reshape(n * cap, feature), text.reshape(n * cap, feature))
    return pl.pallas_call(
        functools.partial(place_kernel, n, block, cap + 1),
        out_shape=(half, half),
        in_specs=[pl.BlockSpec(memory_space=pltpu.SMEM), anywhere, anywhere],
        out_specs=(anywhere, anywhere),
        scratch_shapes=[slots, slots, dma((4, n))],
    )(meta, got_img, got_txt)


def solution(mesh):
    return jax.shard_map(
        shards,
        mesh=mesh,
        in_specs=(
            P(("groups", "docs"), None),
            P("groups"),
            P(("groups", "docs"), None),
            P(("groups", "docs"), None),
            P(("groups", "docs")),
            P(("groups", "docs"), None),
        ),
        out_specs=(P(("groups", "docs"), None), P(("groups", "docs"), None)),
        check_vma=False,
    )
```
